32 devices in a mesh: grp: 2 (over y), lon: 4 (over z), lat: 2 (over x), lvl: 2 (over core).
Axes of the slice: x: 2, y: 2, z: 4, core: 2. Of those that a mesh axis runs over, the one named last changes fastest.
Arguments:
- tokens: bfloat16 [4, 24, 96, 512], P(('grp', 'lvl'), 'lat', 'lon'), parts along dimension 0, may hold values from -8 to 8
- fine_tags: int32 [4, 24, 96], P(('grp', 'lvl'), 'lat', 'lon'), parts along dimension 0, may hold values from 1 to 3
- coarse_tags: int32 [4, 12, 48], P(('grp', 'lvl'), 'lat', 'lon'), parts along dimension 0, may hold values from 1 to 3
- fine_gain: float32 [512], replicated, may hold values from 0.25 to 1.75
- fine_inward: bfloat16 [3, 512, 512], P(None, 'lon', 'lvl'), may hold values from -0.25 to 0.25
- fine_outward: bfloat16 [512, 512], P('lon', 'lvl'), may hold values from -0.25 to 0.25
- fine_table: float32 [16, 253], replicated, may hold values from -2 to 300
- merge_gain: float32 [2048], replicated, may hold values from 0.25 to 1.75
- merge_weight: bfloat16 [1024, 2048], P('lon', 'lvl'), may hold values from -0.125 to 0.125
- coarse_gain: float32 [1024], replicated, may hold values from 0.25 to 1.75
- coarse_inward: bfloat16 [3, 1024, 1024], P(None, 'lon', 'lvl'), may hold values from -0.1875 to 0.1875
- coarse_outward: bfloat16 [1024, 1024], P('lon', 'lvl'), may hold values from -0.1875 to 0.1875
- coarse_table: float32 [32, 253], replicated, may hold values from -2 to 300
Outputs:
- fine_out: bfloat16 [4, 24, 96, 512], P(('grp', 'lvl'), 'lat', 'lon'), parts along dimension 0
- coarse_out: bfloat16 [4, 12, 48, 1024], P(('grp', 'lvl'), 'lat', 'lon'), parts along dimension 0
The draws below stay inside these ranges and needn't reach their ends.
There are 2 independent parts, one for each index of `grp`. The reference program is written for one: setup_inputs(seed, part) draws one part's arguments, and reference() takes and returns one part's arrays. A program takes and returns all parts, laid end to end along the dimension named above; an argument that names none is the same for every part. Nothing has to cross between parts.
All inputs are finite; a program needn't handle non-finite values.
Results may differ from the reference program's by a relative error of at most 0.017.
Values may be sent and summed in bfloat16 or wider, within the bound.
A program may use at most 64 MiB of HBM per device.

```python
import jax
import jax.numpy as jnp
from jax import lax

D1 = 512
HEADS1 = 16
D2 = 1024
HEADS2 = 32
WIN_LAT = 6
WIN_LON = 12
LEVELS = 2
LATS = 24
LONS = 96


def draw_tokens(key, part):
    normal_key = jax.random.fold_in(key, 0)
    sample = jax.random.normal(normal_key, (LEVELS, LATS, LONS, D1), jnp.float32)
    return jnp.clip(sample, -8.0, 8.0).astype(jnp.float32).astype(jnp.bfloat16)


def table_draw(seed_key, head_count):
    base_key = jax.random.fold_in(seed_key, 0)
    span_lat = 2 * WIN_LAT - 1
    span_lon = 2 * WIN_LON - 1
    baseline = jax.random.uniform(base_key, (head_count, span_lat * span_lon), jnp.float32, -2.0, 2.0)
    return baseline


def draw_fine_table(key, part):
    return table_draw(jax.random.fold_in(key, 11), HEADS1)


def draw_coarse_table(key, part):
    return table_draw(jax.random.fold_in(key, 23), HEADS2)


def with_ends(entries, stream_key, smallest, high):
    longest = entries.shape.index(max(entries.shape))
    spots = []
    for shift in (0, 1):
        where = [jax.random.randint(jax.random.fold_in(stream_key, axis), (), 0, length) for axis, length in enumerate(entries.shape)]
        where[longest] = (where[longest] + shift) % entries.shape[longest]
        spots.append(tuple(where))
    return entries.at[spots[0]].set(smallest).at[spots[1]].set(high)


def level_of(own_key, extent, pieces, least, largest):
    factor_of, own = 1.0, jax.random.fold_in(own_key, 6)
    for position, blocks in pieces:
        steps = jnp.exp(jax.random.uniform(jax.random.fold_in(own, position), (blocks,), jnp.float32, least / len(pieces), largest / len(pieces)))
        factor_of = factor_of * jnp.repeat(steps, extent[position] // blocks).reshape([-1 if axis == position else 1 for axis in range(len(extent))])
    return factor_of


def gaussian(own_key, dims, width, limit, cuts=(), kind=jnp.bfloat16):
    array = width * jax.random.normal(own_key, dims, jnp.float32)
    if cuts:
        array = array * level_of(own_key, dims, cuts, -0.22, 0.18)
    return jnp.clip(array, -limit, limit).astype(kind)


def setup_inputs(seed: int = 0, part: int = 0) -> dict:
    splits = jax.random.split(jax.random.key(seed), 14)
    part_keys = jax.random.split(jax.random.fold_in(splits[13], part), 14)
    tokens = draw_tokens(jax.random.fold_in(jax.random.fold_in(splits[13], part), 71), part)
    fine_tags = with_ends(jax.random.randint(part_keys[1], (LEVELS, LATS, LONS), 1, 4), jax.random.fold_in(part_keys[1], 1), 1, 3).astype(jnp.int32)
    coarse_tags = with_ends(jax.random.randint(part_keys[2], (LEVELS, LATS // 2, LONS // 2), 1, 4), jax.random.fold_in(part_keys[2], 1), 1, 3).astype(jnp.int32)
    fine_gain = jnp.clip(1.0 + 0.15 * jax.random.normal(splits[3], (D1,), jnp.float32), 0.25, 1.75)
    fine_inward = gaussian(splits[4], (3, D1, D1), D1 ** -0.5, 0.25, ((1, 4), (2, 2)))
    fine_outward = gaussian(splits[5], (D1, D1), D1 ** -0.5, 0.25, ((0, 4), (1, 2)))
    fine_table = draw_fine_table(jax.random.fold_in(splits[13], 71), part)
    merge_gain = jnp.clip(1.0 + 0.15 * jax.random.normal(splits[7], (4 * D1,), jnp.float32), 0.25, 1.75)
    merge_weight = gaussian(splits[8], (D2, 4 * D1), (4 * D1) ** -0.5, 0.125, ((0, 4), (1, 2)))
    coarse_gain = jnp.clip(1.0 + 0.15 * jax.random.normal(splits[9], (D2,), jnp.float32), 0.25, 1.75)
    coarse_inward = gaussian(splits[10], (3, D2, D2), D2 ** -0.5, 0.1875, ((1, 4), (2, 2)))
    coarse_outward = gaussian(splits[11], (D2, D2), D2 ** -0.5, 0.1875, ((0, 4), (1, 2)))
    coarse_table = draw_coarse_table(jax.random.fold_in(splits[13], 71), part)
    return dict(tokens=tokens, fine_tags=fine_tags, coarse_tags=coarse_tags, fine_gain=fine_gain, fine_inward=fine_inward, fine_outward=fine_outward, fine_table=fine_table, merge_gain=merge_gain, merge_weight=merge_weight, coarse_gain=coarse_gain, coarse_inward=coarse_inward, coarse_outward=coarse_outward, coarse_table=coarse_table)


EPSILON = 1e-05

def layer_norm(values, scales):
    widened = values.astype(jnp.float32)
    center = widened - lax.optimization_barrier(jnp.mean(widened, axis=-1, keepdims=True))
    spread = lax.optimization_barrier(jnp.mean(center * center, axis=-1, keepdims=True))
    return center * lax.rsqrt(spread + EPSILON) * scales.astype(jnp.float32)

def bias_blocks(bias_table, win_lat, win_lon):
    head_count = bias_table.shape[0]
    span_lat = 2 * win_lat - 1
    span_lon = 2 * win_lon - 1
    table_grid = bias_table.astype(jnp.float32).reshape(head_count, span_lat, span_lon)
    lat_pos = jnp.arange(win_lat)
    lon_pos = jnp.arange(win_lon)
    lat_onehot = (lat_pos[:, None, None] - lat_pos[None, :, None] + win_lat - 1 == jnp.arange(span_lat)[None, None, :]).astype(jnp.float32)
    lon_onehot = (lon_pos[:, None, None] - lon_pos[None, :, None] + win_lon - 1 == jnp.arange(span_lon)[None, None, :]).astype(jnp.float32)
    along_lon = jnp.einsum('hab,ijb->haij', table_grid, lon_onehot, precision=lax.Precision.HIGHEST)
    blocks = jnp.einsum('kla,haij->hkilj', lat_onehot, along_lon, precision=lax.Precision.HIGHEST)
    return blocks.reshape(head_count, win_lat * win_lon, win_lat * win_lon)

def split_windows(array_in, win_lat, win_lon):
    levels, lat_len, lon_len = array_in.shape[:3]
    trailing = array_in.shape[3:]
    blocked = array_in.reshape((levels, lat_len // win_lat, win_lat, lon_len // win_lon, win_lon) + trailing)
    blocked = jnp.moveaxis(blocked, 3, 2)
    return blocked.reshape((levels, lat_len // win_lat, lon_len // win_lon, win_lat * win_lon) + trailing)

def join_windows(array_in, win_lat, win_lon):
    levels, lat_bands, lon_bands = array_in.shape[:3]
    trailing = array_in.shape[4:]
    blocked = array_in.reshape((levels, lat_bands, lon_bands, win_lat, win_lon) + trailing)
    blocked = jnp.moveaxis(blocked, 3, 2)
    return blocked.reshape((levels, lat_bands * win_lat, lon_bands * win_lon) + trailing)

def attend(query_grid, key_grid, value_grid, tag_grid, bias_table, win_lat, win_lon):
    head_count = bias_table.shape[0]
    features = query_grid.shape[-1]
    head_size = features // head_count
    offsets_bias = bias_blocks(bias_table, win_lat, win_lon)

    def heads_of(array_in):
        blocks = split_windows(array_in, win_lat, win_lon)
        return blocks.reshape((-1,) + blocks.shape[2:4] + (head_count, head_size)).astype(jnp.float32)
    query_heads = heads_of(query_grid)
    key_heads = heads_of(key_grid)
    value_heads = heads_of(value_grid)
    tag_blocks = split_windows(tag_grid, win_lat, win_lon)
    tag_blocks = tag_blocks.reshape((-1,) + tag_blocks.shape[2:4])

    def one_band(inputs):
        query_band, key_band, value_band, tag_band = inputs
        scores = jnp.einsum('bphd,bqhd->bhpq', query_band, key_band, precision=lax.Precision.HIGHEST)
        scores = scores * head_size ** (-0.5) + offsets_bias
        allowed = tag_band[:, None, :, None] == tag_band[:, None, None, :]
        scores = jnp.where(allowed, scores, -jnp.inf)
        highest = lax.optimization_barrier(jnp.max(scores, axis=-1, keepdims=True))
        weights = jnp.exp(scores - highest)
        shares = (weights / lax.optimization_barrier(jnp.sum(weights, axis=-1, keepdims=True))).astype(jnp.bfloat16)
        blended = jnp.einsum('bhpq,bqhd->bphd', shares.astype(jnp.float32), value_band, precision=lax.Precision.HIGHEST)
        return blended.astype(jnp.bfloat16).reshape(blended.shape[:2] + (features,))
    blended = lax.map(one_band, (query_heads, key_heads, value_heads, tag_blocks))
    levels, lat_len = query_grid.shape[:2]
    blended = blended.reshape((levels, lat_len // win_lat) + blended.shape[1:])
    return join_windows(blended, win_lat, win_lon)

def window_block(stream, tag_grid, gain_row, inward, outward, bias_table):
    levels, lat_len, lon_len, features = stream.shape
    normed = layer_norm(stream, gain_row).astype(jnp.bfloat16)
    flattened = normed.reshape(-1, features)
    lat_half = WIN_LAT // 2
    lon_half = WIN_LON // 2

    def arrange(array_in):
        rolled = jnp.roll(array_in, -lon_half, axis=2)
        padding = [(0, 0), (lat_half, lat_half)] + [(0, 0)] * (array_in.ndim - 2)
        return jnp.pad(rolled, padding)
    projected = []
    for member in range(3):
        product = jnp.dot(flattened, inward[member], preferred_element_type=jnp.float32).astype(jnp.bfloat16)
        projected.append(arrange(product.reshape(levels, lat_len, lon_len, features)))
    blended = attend(projected[0], projected[1], projected[2], arrange(tag_grid), bias_table, WIN_LAT, WIN_LON)
    blended = jnp.roll(blended[:, lat_half:lat_half + lat_len], lon_half, axis=2)
    update = jnp.dot(blended.reshape(-1, features), outward.T, preferred_element_type=jnp.float32)
    return (stream.astype(jnp.float32) + update.reshape(stream.shape)).astype(jnp.bfloat16)

def group_patches(stream):
    levels, lat_len, lon_len, features = stream.shape
    blocked = stream.reshape(levels, lat_len // 2, 2, lon_len // 2, 2, features)
    blocked = jnp.moveaxis(blocked, 3, 2)
    return blocked.reshape(levels, lat_len // 2, lon_len // 2, 4 * features)

def reference(tokens, fine_tags, coarse_tags, fine_gain, fine_inward, fine_outward, fine_table, merge_gain, merge_weight, coarse_gain, coarse_inward, coarse_outward, coarse_table):
    fine_result = window_block(tokens, fine_tags, fine_gain, fine_inward, fine_outward, fine_table)
    grouped = group_patches(fine_result)
    merged_normed = layer_norm(grouped, merge_gain).astype(jnp.bfloat16)
    levels, lat_len, lon_len, wide_features = merged_normed.shape
    coarse_in = jnp.dot(merged_normed.reshape(-1, wide_features), merge_weight.T, preferred_element_type=jnp.float32)
    coarse_in = coarse_in.astype(jnp.bfloat16).reshape(levels, lat_len, lon_len, -1)
    coarse_result = window_block(coarse_in, coarse_tags, coarse_gain, coarse_inward, coarse_outward, coarse_table)
    return (fine_result, coarse_result)
```

```python
import functools

import jax
import jax.numpy as jnp
import numpy as np
from jax import lax
from jax.experimental import pallas as pl
from jax.experimental.pallas import tpu as pltpu
from jax.sharding import PartitionSpec as P

WIN_LAT = 6
WIN_LON = 12
HALF_LAT = WIN_LAT // 2
HALF_LON = WIN_LON // 2
WIN = WIN_LAT * WIN_LON
EPSILON = 1e-05
LANES = 128
MESH = pl.DeviceIdType.MESH
VMEM = pl.BlockSpec(memory_space=pltpu.VMEM)
ANY = pl.BlockSpec(memory_space=pl.ANY)
LIMIT = 60 * 1024 * 1024
NT = (((1,), (1,)), ((), ()))
AROUND = ((0, -1), (0, 1), (-1, 0), (1, 0), (-1, -1), (-1, 1), (1, -1), (1, 1))


def up_to(count, step):
    return -(-count // step) * step


ROWS = up_to(WIN, 16)


class Plan:
    def __init__(self, lat_len, lon_len):
        self.lat_len, self.lon_len = lat_len, lon_len
        self.own = lat_len * lon_len
        self.own_rows = up_to(self.own, 16)
        self.segments = {}
        offset = self.own_rows
        for side in AROUND:
            count = self.extent(side)
            self.segments[side] = (offset, up_to(count, 16))
            offset += up_to(count, 16)
        self.wide_rows = offset
        self.bands = lat_len // WIN_LAT + 1
        self.columns = lon_len // WIN_LON + 1
        self.windows = self.bands * self.columns
        gather = np.full((self.windows * ROWS, 1), -1, np.int32)
        scatter = np.full((self.own_rows, 1), -1, np.int32)
        for w in range(self.windows):
            band, col = divmod(w, self.columns)
            for p in range(WIN):
                r = band * WIN_LAT - HALF_LAT + p // WIN_LON
                c = col * WIN_LON - HALF_LON + p % WIN_LON
                dy = -1 if r < 0 else int(r >= lat_len)
                dx = -1 if c < 0 else int(c >= lon_len)
                if dy == 0 and dx == 0:
                    gather[w * ROWS + p] = r * lon_len + c
                    scatter[r * lon_len + c] = w * ROWS + p
                    continue
                width = HALF_LON if dx else lon_len
                rr = r + HALF_LAT if dy < 0 else (r - lat_len if dy > 0 else r)
                cc = c + HALF_LON if dx < 0 else (c - lon_len if dx > 0 else c)
                gather[w * ROWS + p] = self.segments[(dy, dx)][0] + rr * width + cc
        self.gather, self.scatter = gather, scatter

    def extent(self, side):
        rows = HALF_LAT if side[0] else self.lat_len
        cols = HALF_LON if side[1] else self.lon_len
        return rows * cols

    def edges(self):
        result = np.full((self.wide_rows - self.own_rows, 1), -1, np.int32)
        for dy, dx in AROUND:
            offset = self.segments[(dy, dx)][0] - self.own_rows
            rows = range(self.lat_len)
            rows = rows[-HALF_LAT:] if dy < 0 else (rows[:HALF_LAT] if dy > 0 else rows)
            cols = range(self.lon_len)
            cols = cols[-HALF_LON:] if dx < 0 else (cols[:HALF_LON] if dx > 0 else cols)
            for i, (r, c) in enumerate((r, c) for r in rows for c in cols):
                result[offset + i] = r * self.lon_len + c
        return result

    def patches(self):
        half_lat, half_lon = self.lat_len // 2, self.lon_len // 2
        result = np.full((4, up_to(half_lat * half_lon, 16), 1), -1, np.int32)
        for s in range(2):
            for t in range(2):
                for a in range(half_lat):
                    for b in range(half_lon):
                        result[2 * s + t, a * half_lon + b] = (2 * a + s) * self.lon_len + 2 * b + t
        return result


def onehot(index, width):
    spots = lax.broadcasted_iota(jnp.int32, (index.shape[0], width), 1)
    return jnp.where(spots == index, 1.0, 0.0).astype(jnp.bfloat16)


def pick(index, source):
    return jnp.dot(
        onehot(index, source.shape[0]), source, preferred_element_type=jnp.float32
    ).astype(jnp.bfloat16)


def normalize(values, gain):
    widened = values.astype(jnp.float32)
    center = widened - jnp.mean(widened, axis=-1, keepdims=True)
    spread = jnp.mean(center * center, axis=-1, keepdims=True)
    return (center * lax.rsqrt(spread + EPSILON) * gain).astype(jnp.bfloat16)


def exchange_halo(plan, edge_ref, wide, send_sem, recv_sem):
    lat, lon = lax.axis_index("lat"), lax.axis_index("lon")
    lats, lons = lax.axis_size("lat"), lax.axis_size("lon")

    def place(dy, dx):
        return {"lat": lax.rem(lat + dy + lats, lats), "lon": lax.rem(lon + dx + lons, lons)}

    def when_there(dy, action):
        if dy == 0:
            action()
        else:
            pl.when((lat > 0) if dy < 0 else (lat < lats - 1))(action)

    barrier = pltpu.get_barrier_semaphore()
    for dy, dx in AROUND:
        def greet(dy=dy, dx=dx):
            pl.semaphore_signal(barrier, inc=1, device_id=place(dy, dx), device_id_type=MESH)
        when_there(dy, greet)
    peers = 2 + 3 * (lat > 0).astype(jnp.int32) + 3 * (lat < lats - 1).astype(jnp.int32)
    pl.semaphore_wait(barrier, peers)

    def copy_of(number, dy, dx):
        offset, count = plan.segments[(dy, dx)]
        return pltpu.make_async_remote_copy(
            src_ref=edge_ref.at[pl.ds(offset - plan.own_rows, count)],
            dst_ref=wide.at[pl.ds(offset, count)],
            send_sem=send_sem.at[number],
            recv_sem=recv_sem.at[number],
            device_id=place(-dy, -dx),
            device_id_type=MESH,
        )

    for number, (dy, dx) in enumerate(AROUND):
        when_there(-dy, lambda n=number, y=dy, x=dx: copy_of(n, y, x).start())
        if dy:
            offset, count = plan.segments[(dy, dx)]

            def clear(offset=offset, count=count):
                wide[pl.ds(offset, count), :] = jnp.zeros((count, wide.shape[1]), wide.dtype)

            pl.when(jnp.logical_not((lat > 0) if dy < 0 else (lat < lats - 1)))(clear)

    def finish():
        for number, (dy, dx) in enumerate(AROUND):
            when_there(dy, lambda n=number, y=dy, x=dx: copy_of(n, y, x).wait_recv())
            when_there(-dy, lambda n=number, y=dy, x=dx: copy_of(n, y, x).wait_send())

    return finish


def attend_windows(plan, wide, gather_ref, gain_ref, inward_ref, bias_ref, normed, triple, tags, mixed):
    features = normed.shape[1]
    heads = bias_ref.shape[0]
    size = features // heads
    per_group = LANES // size
    groups = features // LANES
    everything = wide[...]

    for w in range(plan.windows):
        rows = pl.ds(w * ROWS, ROWS)
        chosen = pick(gather_ref[rows, :], everything)
        normed[rows, :] = normalize(chosen[:, :features], gain_ref[...])
        tags[rows, :] = chosen[:, features:]

    step = 256
    for member in range(3):
        @pl.loop(0, features // step)
        def _(block):
            cols = pl.ds(pl.multiple_of(block * step, step), step)
            triple[member, :, cols] = jnp.dot(
                normed[...], inward_ref[member, :, cols], preferred_element_type=jnp.float32
            ).astype(jnp.bfloat16)

    owner = lax.broadcasted_iota(jnp.int32, (ROWS, LANES), 1) // size
    fill = jnp.zeros((LANES - ROWS, LANES), jnp.bfloat16)
    first = jnp.where(
        lax.broadcasted_iota(jnp.int32, (16, LANES), 1) == 0, 1.0, 0.0
    ).astype(jnp.bfloat16)

    def spread(block):
        parts = []
        for h in range(per_group):
            parts += [jnp.where(owner == h, block, jnp.zeros_like(block)), fill]
        return jnp.concatenate(parts, axis=0)

    @pl.loop(0, plan.windows)
    def _(w):
        rows = pl.ds(pl.multiple_of(w * ROWS, ROWS), ROWS)
        tag_block = tags[rows, :]
        across = lax.dot_general(
            first, jnp.concatenate([tag_block, fill], axis=0), NT, preferred_element_type=jnp.float32
        )
        allowed = tag_block[:, :1].astype(jnp.float32) == across[:1, :]

        @pl.loop(0, groups, unroll=2)
        def _(g):
            cols = pl.ds(pl.multiple_of(g * LANES, LANES), LANES)
            keys = spread(triple[1, rows, cols])
            scores = lax.dot_general(
                triple[0, rows, cols], keys, NT, preferred_element_type=jnp.float32
            )
            shares = []
            for h in range(per_group):
                score = scores[:, h * LANES : (h + 1) * LANES] * size ** (-0.5)
                score = score + bias_ref[g * per_group + h]
                score = jnp.where(allowed, score, -1e30)
                weight = jnp.exp(score - jnp.max(score, axis=-1, keepdims=True))
                total = jnp.sum(weight, axis=-1, keepdims=True)
                shares.append((weight * (1.0 / total)).astype(jnp.bfloat16))
            blended = jnp.dot(
                jnp.concatenate(shares, axis=1),
                spread(triple[2, rows, cols]),
                preferred_element_type=jnp.float32,
            )
            mixed[rows, cols] = blended.astype(jnp.bfloat16)


def fine_kernel(
    plan, own_ref, edge_ref, tag_ref, gather_ref, scatter_ref, patch_ref, edge_index_ref, gain_ref,
    inward_ref, outward_ref, bias_ref, merge_gain_ref, merge_ref,
    fine_ref, coarse_ref, coarse_edge_ref, wide, normed, triple, tags, mixed, send_sem, recv_sem,
):
    features = normed.shape[1]
    finish = exchange_halo(plan, edge_ref, wide, send_sem, recv_sem)
    wide[: plan.own_rows, :] = own_ref[...]
    finish()
    attend_windows(plan, wide, gather_ref, gain_ref, inward_ref, bias_ref, normed, triple, tags, mixed)
    own_mixed = pick(scatter_ref[...], mixed[...])
    update = lax.dot_general(own_mixed, outward_ref[0], NT, preferred_element_type=jnp.float32)
    fine = (own_ref[:, :features].astype(jnp.float32) + update).astype(jnp.bfloat16)
    fine_ref[...] = fine
    members = [pick(patch_ref[m], fine).astype(jnp.float32) for m in range(4)]
    count = 4 * features
    mean = sum(jnp.sum(m, axis=-1, keepdims=True) for m in members) / count
    centers = [m - mean for m in members]
    spread = sum(jnp.sum(c * c, axis=-1, keepdims=True) for c in centers) / count
    factor = lax.rsqrt(spread + EPSILON)
    merged = None
    for m in range(4):
        cols = slice(m * features, (m + 1) * features)
        part = (centers[m] * factor * merge_gain_ref[:, cols]).astype(jnp.bfloat16)
        term = lax.dot_general(part, merge_ref[0, :, cols], NT, preferred_element_type=jnp.float32)
        merged = term if merged is None else merged + term
    coarse = jnp.concatenate([merged.astype(jnp.bfloat16), tag_ref[...]], axis=1)
    coarse_ref[...] = coarse
    coarse_edge_ref[...] = pick(edge_index_ref[...], coarse)


def coarse_kernel(
    plan, own_ref, edge_ref, gather_ref, scatter_ref, gain_ref, inward_ref, outward_ref, bias_ref,
    out_ref, wide, normed, triple, tags, mixed, send_sem, recv_sem,
):
    features = normed.shape[1]
    finish = exchange_halo(plan, edge_ref, wide, send_sem, recv_sem)
    wide[: plan.own_rows, :] = own_ref[...]
    finish()
    attend_windows(plan, wide, gather_ref, gain_ref, inward_ref, bias_ref, normed, triple, tags, mixed)
    own_mixed = pick(scatter_ref[...], mixed[...])
    update = lax.dot_general(own_mixed, outward_ref[0], NT, preferred_element_type=jnp.float32)
    out_ref[...] = (own_ref[:, :features].astype(jnp.float32) + update).astype(jnp.bfloat16)


def level_scratch(plan, features):
    rows = plan.windows * ROWS
    return [
        pltpu.VMEM((plan.wide_rows, features + LANES), jnp.bfloat16),
        pltpu.VMEM((rows, features), jnp.bfloat16),
        pltpu.VMEM((3, rows, features), jnp.bfloat16),
        pltpu.VMEM((rows, LANES), jnp.bfloat16),
        pltpu.VMEM((rows, features), jnp.bfloat16),
        pltpu.SemaphoreType.DMA((len(AROUND),)),
        pltpu.SemaphoreType.DMA((len(AROUND),)),
    ]


def gather_kernel(count, split, *refs):
    shards, fulls = refs[:count], refs[count : 2 * count]
    (local_sem, lon_send, lon_recv, one_send, one_recv, two_send, two_recv, lvl_send, lvl_recv) = refs[2 * count :]
    grp, lat, lon, lvl = (lax.axis_index(a) for a in ("grp", "lat", "lon", "lvl"))
    grps, lats, lons, lvls = (lax.axis_size(a) for a in ("grp", "lat", "lon", "lvl"))
    halves = 2 if split else 1

    def at(axis, index, size, step):
        return {axis: lax.rem(index + step, size)}

    greeted = [at("lon", lon, lons, d) for d in range(1, lons)]
    if split:
        greeted += [at("lat", lat, lats, d) for d in range(1, lats)]
        greeted += [at("grp", grp, grps, d) for d in range(1, grps)]
    greeted += [at("lvl", lvl, lvls, d) for d in range(1, lvls)]
    barrier = pltpu.get_barrier_semaphore()
    for device in greeted:
        pl.semaphore_signal(barrier, inc=1, device_id=device, device_id_type=MESH)
    pl.semaphore_wait(barrier, len(greeted))

    def place(m, lon_of, lvl_of, start, size):
        rows, cols = shards[m].shape[1:]
        return fulls[m].at[
            :, pl.ds(pl.multiple_of(lon_of * rows + start, 16), size), pl.ds(pl.multiple_of(lvl_of * cols, cols), cols)
        ]

    def remote(src, dst, send, recv, device):
        return pltpu.make_async_remote_copy(
            src_ref=src, dst_ref=dst, send_sem=send, recv_sem=recv, device_id=device, device_id_type=MESH
        )

    def piece(m, half, grp_of, lat_of):
        rows = shards[m].shape[1]
        if not split:
            return 0, rows
        size = rows // (2 * grps * lats)
        order = grp_of * lats + lat_of if half == 0 else lat_of * grps + grp_of
        return half * (rows // 2) + order * size, size

    def own_copy(m):
        rows = shards[m].shape[1]
        return pltpu.make_async_copy(shards[m], place(m, lon, lvl, 0, rows), local_sem.at[m])

    def lon_copy(m, d, half):
        start, size = piece(m, half, grp, lat)
        return remote(
            shards[m].at[:, pl.ds(start if isinstance(start, int) else pl.multiple_of(start, 16), size), :],
            place(m, lon, lvl, start, size),
            lon_send.at[m, d - 1, half], lon_recv.at[m, d - 1, half], at("lon", lon, lons, d),
        )

    def plane(half, first):
        by_lat = (half == 0) == first
        return ("lat", lat, lats) if by_lat else ("grp", grp, grps)

    def one_copy(m, d, half, e):
        source = lax.rem(lon - d + lons, lons)
        start, size = piece(m, half, grp, lat)
        block = place(m, source, lvl, start, size)
        return remote(block, block, one_send.at[m, d - 1, half, e - 1], one_recv.at[m, d - 1, half, e - 1], at(*plane(half, True), e))

    def two_copy(m, d, half, e):
        source = lax.rem(lon - d + lons, lons)
        if half == 0:
            start, size = piece(m, half, grp, 0)
            size *= lats
        else:
            start, size = piece(m, half, 0, lat)
            size *= grps
        block = place(m, source, lvl, start, size)
        return remote(block, block, two_send.at[m, d - 1, half, e - 1], two_recv.at[m, d - 1, half, e - 1], at(*plane(half, False), e))

    def lvl_copy(m, d, e):
        rows = shards[m].shape[1]
        source = lax.rem(lon - d + lons, lons)
        block = place(m, source, lvl, 0, rows)
        return remote(
            shards[m] if d == 0 else block, block,
            lvl_send.at[m, d, e - 1], lvl_recv.at[m, d, e - 1], at("lvl", lvl, lvls, e),
        )

    ways = [(d, half) for d in range(1, lons) for half in range(halves)]
    for m in range(count):
        own_copy(m).start()
        for d, half in ways:
            lon_copy(m, d, half).start()
        for e in range(1, lvls):
            lvl_copy(m, 0, e).start()

    def others(half, first):
        return range(1, plane(half, first)[2])

    def share_one(m):
        for d, half in ways:
            lon_copy(m, d, half).wait_recv()
            if split:
                for e in others(half, True):
                    one_copy(m, d, half, e).start()

    def share_two(m):
        for d, half in ways:
            if split:
                for e in others(half, True):
                    one_copy(m, d, half, e).wait_recv()
                for e in others(half, False):
                    two_copy(m, d, half, e).start()

    def share_lvl(m):
        for d in range(1, lons):
            if split:
                for half in range(halves):
                    for e in others(half, False):
                        two_copy(m, d, half, e).wait_recv()
            for e in range(1, lvls):
                lvl_copy(m, d, e).start()

    for s in range(count + 2):
        if s < count:
            share_one(s)
        if 0 <= s - 1 < count:
            share_two(s - 1)
        if 0 <= s - 2 < count:
            share_lvl(s - 2)
    for m in range(count):
        own_copy(m).wait()
        for d in range(lons):
            for e in range(1, lvls):
                lvl_copy(m, d, e).wait()
        for d, half in ways:
            lon_copy(m, d, half).wait_send()
            if split:
                for e in others(half, True):
                    one_copy(m, d, half, e).wait_send()
                for e in others(half, False):
                    two_copy(m, d, half, e).wait_send()


def gather_weights(weights):
    grps, lats, lons, lvls = (lax.axis_size(a) for a in ("grp", "lat", "lon", "lvl"))
    split = all(w.shape[1] % (2 * grps * lats * 16) == 0 for w in weights)
    count = len(weights)
    halves = 2 if split else 1
    dma = pltpu.SemaphoreType.DMA
    most = max(grps, lats) - 1 if split else 1
    return pl.pallas_call(
        functools.partial(gather_kernel, count, split),
        out_shape=[
            jax.ShapeDtypeStruct((w.shape[0], w.shape[1] * lons, w.shape[2] * lvls), w.dtype) for w in weights
        ],
        in_specs=[ANY] * count,
        out_specs=[VMEM] * count,
        scratch_shapes=[dma((count,))]
        + [dma((count, lons - 1, halves))] * 2
        + [dma((count, lons - 1, halves, most))] * 4
        + [dma((count, lons, lvls - 1))] * 2,
        compiler_params=pltpu.CompilerParams(collective_id=0, has_side_effects=True, vmem_limit_bytes=LIMIT),
        name="gather_weights",
    )(*weights)


def bias_blocks(table):
    span_lon = 2 * WIN_LON - 1
    p = np.arange(WIN)
    r, c = p // WIN_LON, p % WIN_LON
    number = (r[:, None] - r[None, :] + WIN_LAT - 1) * span_lon + c[:, None] - c[None, :] + WIN_LON - 1
    lat_hot = (r[:, None] - r[None, :] + WIN_LAT - 1)[:, :, None]
    del number
    heads = table.shape[0]
    grid = table.reshape(heads, 2 * WIN_LAT - 1, span_lon)
    i, j = np.arange(WIN_LON)[:, None], np.arange(WIN_LON)[None, :]
    lon_blocks = jnp.stack(
        [lax.slice_in_dim(grid, k, k + WIN_LON, axis=2)[:, :, ::-1] for k in range(WIN_LON)], axis=2
    )
    del lat_hot, i, j
    rows = []
    for k in range(WIN_LAT):
        parts = [lon_blocks[:, k - l + WIN_LAT - 1] for l in range(WIN_LAT)]
        rows.append(jnp.concatenate(parts, axis=2))
    blocks = jnp.concatenate(rows, axis=1)
    return jnp.pad(blocks, ((0, 0), (0, ROWS - WIN), (0, LANES - WIN)))


def shards(
    tokens, fine_tags, coarse_tags, fine_gain, fine_inward, fine_outward, fine_table, merge_gain,
    merge_weight, coarse_gain, coarse_inward, coarse_outward, coarse_table,
):
    _, lat_len, lon_len, width = tokens.shape
    fine_plan, coarse_plan = Plan(lat_len, lon_len), Plan(lat_len // 2, lon_len // 2)
    inward, outward, merge, inward_two, outward_two = gather_weights(
        [fine_inward, fine_outward[None], merge_weight[None], coarse_inward, coarse_outward[None]]
    )
    fine_bias, coarse_bias = bias_blocks(fine_table), bias_blocks(coarse_table)

    tagged = jnp.concatenate(
        [tokens[0], jnp.broadcast_to(fine_tags[0, :, :, None], (lat_len, lon_len, LANES)).astype(jnp.bfloat16)], axis=2
    )
    own = tagged.reshape(lat_len * lon_len, -1)
    own = jnp.pad(own, ((0, fine_plan.own_rows - fine_plan.own), (0, 0)))
    pieces = []
    for dy, dx in AROUND:
        part = tagged
        part = part[-HALF_LAT:] if dy < 0 else (part[:HALF_LAT] if dy > 0 else part)
        part = part[:, -HALF_LON:] if dx < 0 else (part[:, :HALF_LON] if dx > 0 else part)
        part = part.reshape(-1, part.shape[2])
        pieces.append(jnp.pad(part, ((0, up_to(part.shape[0], 16) - part.shape[0]), (0, 0))))
    edge = jnp.concatenate(pieces, axis=0)
    coarse_width = merge.shape[1]
    coarse_marks = jnp.broadcast_to(coarse_tags.reshape(-1, 1), (coarse_plan.own, LANES)).astype(jnp.bfloat16)
    coarse_marks = jnp.pad(coarse_marks, ((0, coarse_plan.own_rows - coarse_plan.own), (0, 0)))

    edge_rows = coarse_plan.wide_rows - coarse_plan.own_rows
    fine, coarse_own, coarse_edge = pl.pallas_call(
        functools.partial(fine_kernel, fine_plan),
        out_shape=[
            jax.ShapeDtypeStruct((fine_plan.own_rows, width), jnp.bfloat16),
            jax.ShapeDtypeStruct((coarse_plan.own_rows, coarse_width + LANES), jnp.bfloat16),
            jax.ShapeDtypeStruct((edge_rows, coarse_width + LANES), jnp.bfloat16),
        ],
        in_specs=[VMEM] * 13,
        out_specs=[VMEM] * 3,
        scratch_shapes=level_scratch(fine_plan, width),
        compiler_params=pltpu.CompilerParams(collective_id=1, has_side_effects=True, vmem_limit_bytes=LIMIT),
        name="fine_level",
    )(
        own, edge, coarse_marks, fine_plan.gather, fine_plan.scatter, fine_plan.patches(),
        coarse_plan.edges(), fine_gain[None], inward, outward, fine_bias, merge_gain[None], merge,
    )
    coarse = pl.pallas_call(
        functools.partial(coarse_kernel, coarse_plan),
        out_shape=jax.ShapeDtypeStruct((coarse_plan.own_rows, coarse_width), jnp.bfloat16),
        in_specs=[VMEM] * 8,
        out_specs=VMEM,
        scratch_shapes=level_scratch(coarse_plan, coarse_width),
        compiler_params=pltpu.CompilerParams(collective_id=2, has_side_effects=True, vmem_limit_bytes=LIMIT),
        name="coarse_level",
    )(
        coarse_own, coarse_edge, coarse_plan.gather, coarse_plan.scatter, coarse_gain[None],
        inward_two, outward_two, coarse_bias,
    )
    fine = fine[: fine_plan.own].reshape(tokens.shape)
    coarse = coarse[: coarse_plan.own].reshape(1, lat_len // 2, lon_len // 2, coarse_width)
    return fine, coarse


def solution(mesh):
    placed = (
        P(("grp", "lvl"), "lat", "lon", None),
        P(("grp", "lvl"), "lat", "lon"),
        P(("grp", "lvl"), "lat", "lon"),
        P(),
        P(None, "lon", "lvl"),
        P("lon", "lvl"),
        P(),
        P(),
        P("lon", "lvl"),
        P(),
        P(None, "lon", "lvl"),
        P("lon", "lvl"),
        P(),
    )
    return jax.shard_map(
        shards,
        mesh=mesh,
        in_specs=placed,
        out_specs=(P(("grp", "lvl"), "lat", "lon", None), P(("grp", "lvl"), "lat", "lon", None)),
        check_vma=False,
    )
```

```python
import functools

import jax
import jax.numpy as jnp
import numpy as np
from jax import lax
from jax.experimental import pallas as pl
from jax.experimental.pallas import tpu as pltpu
from jax.sharding import PartitionSpec as P

WIN_LAT = 6
WIN_LON = 12
HALF_LAT = WIN_LAT // 2
HALF_LON = WIN_LON // 2
WIN = WIN_LAT * WIN_LON
EPSILON = 1e-05
LANES = 128
MESH = pl.DeviceIdType.MESH
VMEM = pl.BlockSpec(memory_space=pltpu.VMEM)
ANY = pl.BlockSpec(memory_space=pl.ANY)
LIMIT = 60 * 1024 * 1024
NT = (((1,), (1,)), ((), ()))
AROUND = ((0, -1), (0, 1), (-1, 0), (1, 0), (-1, -1), (-1, 1), (1, -1), (1, 1))


def up_to(count, step):
    return -(-count // step) * step


ROWS = up_to(WIN, 16)


class Plan:
    def __init__(self, lat_len, lon_len):
        self.lat_len, self.lon_len = lat_len, lon_len
        self.own = lat_len * lon_len
        self.own_rows = up_to(self.own, 16)
        self.segments = {}
        offset = self.own_rows
        for side in AROUND:
            count = self.extent(side)
            self.segments[side] = (offset, up_to(count, 16))
            offset += up_to(count, 16)
        self.wide_rows = offset
        self.bands = lat_len // WIN_LAT + 1
        self.columns = lon_len // WIN_LON + 1
        self.windows = self.bands * self.columns
        gather = np.full((self.windows * ROWS, 1), -1, np.int32)
        scatter = np.full((self.own_rows, 1), -1, np.int32)
        for w in range(self.windows):
            band, col = divmod(w, self.columns)
            for p in range(WIN):
                r = band * WIN_LAT - HALF_LAT + p // WIN_LON
                c = col * WIN_LON - HALF_LON + p % WIN_LON
                dy = -1 if r < 0 else int(r >= lat_len)
                dx = -1 if c < 0 else int(c >= lon_len)
                if dy == 0 and dx == 0:
                    gather[w * ROWS + p] = r * lon_len + c
                    scatter[r * lon_len + c] = w * ROWS + p
                    continue
                width = HALF_LON if dx else lon_len
                rr = r + HALF_LAT if dy < 0 else (r - lat_len if dy > 0 else r)
                cc = c + HALF_LON if dx < 0 else (c - lon_len if dx > 0 else c)
                gather[w * ROWS + p] = self.segments[(dy, dx)][0] + rr * width + cc
        self.gather, self.scatter = gather, scatter

    def extent(self, side):
        rows = HALF_LAT if side[0] else self.lat_len
        cols = HALF_LON if side[1] else self.lon_len
        return rows * cols

    def edges(self):
        result = np.full((self.wide_rows - self.own_rows, 1), -1, np.int32)
        for dy, dx in AROUND:
            offset = self.segments[(dy, dx)][0] - self.own_rows
            rows = range(self.lat_len)
            rows = rows[-HALF_LAT:] if dy < 0 else (rows[:HALF_LAT] if dy > 0 else rows)
            cols = range(self.lon_len)
            cols = cols[-HALF_LON:] if dx < 0 else (cols[:HALF_LON] if dx > 0 else cols)
            for i, (r, c) in enumerate((r, c) for r in rows for c in cols):
                result[offset + i] = r * self.lon_len + c
        return result

    def patches(self):
        half_lat, half_lon = self.lat_len // 2, self.lon_len // 2
        result = np.full((4, up_to(half_lat * half_lon, 16), 1), -1, np.int32)
        for s in range(2):
            for t in range(2):
                for a in range(half_lat):
                    for b in range(half_lon):
                        result[2 * s + t, a * half_lon + b] = (2 * a + s) * self.lon_len + 2 * b + t
        return result


def onehot(index, width):
    spots = lax.broadcasted_iota(jnp.int32, (index.shape[0], width), 1)
    return jnp.where(spots == index, 1.0, 0.0).astype(jnp.bfloat16)


def pick(index, source):
    return jnp.dot(
        onehot(index, source.shape[0]), source, preferred_element_type=jnp.float32
    ).astype(jnp.bfloat16)


def normalize(values, gain):
    widened = values.astype(jnp.float32)
    center = widened - jnp.mean(widened, axis=-1, keepdims=True)
    spread = jnp.mean(center * center, axis=-1, keepdims=True)
    return (center * lax.rsqrt(spread + EPSILON) * gain).astype(jnp.bfloat16)


def exchange_halo(plan, edge_ref, wide, send_sem, recv_sem, greeted=()):
    lat, lon = lax.axis_index("lat"), lax.axis_index("lon")
    lats, lons = lax.axis_size("lat"), lax.axis_size("lon")

    def place(dy, dx):
        return {"lat": lax.rem(lat + dy + lats, lats), "lon": lax.rem(lon + dx + lons, lons)}

    def when_there(dy, action):
        if dy == 0:
            action()
        else:
            pl.when((lat > 0) if dy < 0 else (lat < lats - 1))(action)

    barrier = pltpu.get_barrier_semaphore()
    for dy, dx in AROUND:
        def greet(dy=dy, dx=dx):
            pl.semaphore_signal(barrier, inc=1, device_id=place(dy, dx), device_id_type=MESH)
        when_there(dy, greet)
    peers = 2 + 3 * (lat > 0).astype(jnp.int32) + 3 * (lat < lats - 1).astype(jnp.int32)
    for device in greeted:
        pl.semaphore_signal(barrier, inc=1, device_id=device, device_id_type=MESH)
    pl.semaphore_wait(barrier, peers + len(greeted))

    def copy_of(number, dy, dx):
        offset, count = plan.segments[(dy, dx)]
        return pltpu.make_async_remote_copy(
            src_ref=edge_ref.at[pl.ds(offset - plan.own_rows, count)],
            dst_ref=wide.at[pl.ds(offset, count)],
            send_sem=send_sem.at[number],
            recv_sem=recv_sem.at[number],
            device_id=place(-dy, -dx),
            device_id_type=MESH,
        )

    for number, (dy, dx) in enumerate(AROUND):
        when_there(-dy, lambda n=number, y=dy, x=dx: copy_of(n, y, x).start())
        if dy:
            offset, count = plan.segments[(dy, dx)]

            def clear(offset=offset, count=count):
                wide[pl.ds(offset, count), :] = jnp.zeros((count, wide.shape[1]), wide.dtype)

            pl.when(jnp.logical_not((lat > 0) if dy < 0 else (lat < lats - 1)))(clear)

    def finish():
        for number, (dy, dx) in enumerate(AROUND):
            when_there(dy, lambda n=number, y=dy, x=dx: copy_of(n, y, x).wait_recv())
            when_there(-dy, lambda n=number, y=dy, x=dx: copy_of(n, y, x).wait_send())

    return finish


def fill_bias(number_ref, parts_ref, bias):
    heads = bias.shape[0]
    entries = parts_ref.shape[1]
    parts = parts_ref[...]
    spots = lax.broadcasted_iota(jnp.int32, (entries, LANES), 0)
    for p in range(WIN):
        hot = jnp.where(spots == number_ref[p : p + 1, :], 1.0, 0.0).astype(jnp.bfloat16)
        terms = jnp.dot(parts, hot, preferred_element_type=jnp.float32)
        bias[:, p, :] = terms[:heads] + terms[heads : 2 * heads] + terms[2 * heads :]
    bias[:, WIN:, :] = jnp.zeros((heads, ROWS - WIN, LANES), jnp.float32)


def arrange_windows(plan, wide, gather_ref, gain_ref, normed, tags):
    features = normed.shape[1]
    everything = wide[...]
    for w in range(plan.windows):
        rows = pl.ds(w * ROWS, ROWS)
        chosen = pick(gather_ref[rows, :], everything)
        normed[rows, :] = normalize(chosen[:, :features], gain_ref[...])
        tags[rows, :] = chosen[:, features:]


def attend_windows(plan, inward_ref, bias_ref, normed, triple, tags, mixed, unroll, after=None):
    features = normed.shape[1]
    heads = bias_ref.shape[0]
    size = features // heads
    per_group = LANES // size
    groups = features // LANES

    step = 256
    for member in range(3):
        @pl.loop(0, features // step)
        def _(block):
            cols = pl.ds(pl.multiple_of(block * step, step), step)
            triple[member, :, cols] = jnp.dot(
                normed[...], inward_ref[member, :, cols], preferred_element_type=jnp.float32
            ).astype(jnp.bfloat16)

    owner = lax.broadcasted_iota(jnp.int32, (ROWS, LANES), 1) // size
    fill = jnp.zeros((LANES - ROWS, LANES), jnp.bfloat16)
    first = jnp.where(
        lax.broadcasted_iota(jnp.int32, (16, LANES), 1) == 0, 1.0, 0.0
    ).astype(jnp.bfloat16)

    def spread(block):
        parts = []
        for h in range(per_group):
            parts += [jnp.where(owner == h, block, jnp.zeros_like(block)), fill]
        return jnp.concatenate(parts, axis=0)

    head_of_row = lax.broadcasted_iota(jnp.int32, (per_group * LANES, LANES), 0) // LANES
    head_of_lane = lax.broadcasted_iota(jnp.int32, (per_group * LANES, LANES), 1) // size
    ones = jnp.where(head_of_row == head_of_lane, 1.0, 0.0).astype(jnp.bfloat16)

    @pl.loop(0, plan.windows)
    def _(w):
        rows = pl.ds(pl.multiple_of(w * ROWS, ROWS), ROWS)
        tag_block = tags[rows, :]
        across = lax.dot_general(
            first, jnp.concatenate([tag_block, fill], axis=0), NT, preferred_element_type=jnp.float32
        )
        allowed = tag_block[:, :1].astype(jnp.float32) == across[:1, :]

        @pl.loop(0, groups, unroll=unroll)
        def _(g):
            cols = pl.ds(pl.multiple_of(g * LANES, LANES), LANES)
            scores = lax.dot_general(
                triple[0, rows, cols], spread(triple[1, rows, cols]), NT, preferred_element_type=jnp.float32
            )
            weights = []
            for h in range(per_group):
                score = scores[:, h * LANES : (h + 1) * LANES] * size ** (-0.5)
                score = score + bias_ref[g * per_group + h]
                score = jnp.where(allowed, score, -1e30)
                weight = jnp.exp(score - jnp.max(score, axis=-1, keepdims=True))
                weights.append(weight.astype(jnp.bfloat16))
            weights = jnp.concatenate(weights, axis=1)
            blended = jnp.dot(weights, spread(triple[2, rows, cols]), preferred_element_type=jnp.float32)
            totals = jnp.dot(weights, ones, preferred_element_type=jnp.float32)
            mixed[rows, cols] = (blended / totals).astype(jnp.bfloat16)

        if after is not None:
            after(w)


def fine_kernel(
    plan, split, own_ref, edge_ref, tag_ref, gather_ref, scatter_ref, patch_ref, edge_index_ref, gain_ref,
    number_ref, parts_ref, coarse_parts_ref, merge_gain_ref, s0, s1, s2, s3, s4,
    fine_ref, coarse_ref, coarse_edge_ref, coarse_bias_ref, inward_two_ref, outward_two_ref,
    wide, normed, triple, tags, mixed, send_sem, recv_sem, bias_ref, inward_ref, outward_ref, merge_ref, *sems,
):
    features = normed.shape[1]
    shards = (s0, s1, s2, s3, s4)
    fulls = (inward_ref, outward_ref, merge_ref, inward_two_ref, outward_two_ref)
    gather = Gather(shards, fulls, split, sems)
    finish = exchange_halo(plan, edge_ref, wide, send_sem, recv_sem, gather.greeted())
    gather.begin()
    wide[: plan.own_rows, :] = own_ref[...]
    fill_bias(number_ref, parts_ref, bias_ref)
    finish()
    gather.step(0)
    arrange_windows(plan, wide, gather_ref, gain_ref, normed, tags)
    gather.step(1)
    gather.step(2)
    fill_bias(number_ref, coarse_parts_ref, coarse_bias_ref)
    gather.ready(0)
    last = gather.count + 2
    spots = {}
    for number in range(3, last):
        spots.setdefault(min((number - 3) * plan.windows // (last - 3) + 1, plan.windows - 1), []).append(number)

    def after(w):
        for spot, numbers in spots.items():
            @pl.when(w == spot)
            def _(numbers=numbers):
                for number in numbers:
                    gather.step(number)

    attend_windows(plan, inward_ref, bias_ref, normed, triple, tags, mixed, 2, after)
    gather.ready(1)
    own_mixed = pick(scatter_ref[...], mixed[...])
    update = lax.dot_general(own_mixed, outward_ref[0], NT, preferred_element_type=jnp.float32)
    fine = (own_ref[:, :features].astype(jnp.float32) + update).astype(jnp.bfloat16)
    fine_ref[...] = fine
    gather.ready(2)
    members = [pick(patch_ref[m], fine).astype(jnp.float32) for m in range(4)]
    count = 4 * features
    mean = sum(jnp.sum(m, axis=-1, keepdims=True) for m in members) / count
    centers = [m - mean for m in members]
    spread = sum(jnp.sum(c * c, axis=-1, keepdims=True) for c in centers) / count
    factor = lax.rsqrt(spread + EPSILON)
    merged = None
    for m in range(4):
        cols = slice(m * features, (m + 1) * features)
        part = (centers[m] * factor * merge_gain_ref[:, cols]).astype(jnp.bfloat16)
        term = lax.dot_general(part, merge_ref[0, :, cols], NT, preferred_element_type=jnp.float32)
        merged = term if merged is None else merged + term
    coarse = jnp.concatenate([merged.astype(jnp.bfloat16), tag_ref[...]], axis=1)
    coarse_ref[...] = coarse
    coarse_edge_ref[...] = pick(edge_index_ref[...], coarse)
    for number in range(3, gather.count):
        gather.ready(number)
    gather.end()


def coarse_kernel(
    plan, own_ref, edge_ref, gather_ref, scatter_ref, gain_ref, inward_ref, outward_ref, bias_ref,
    out_ref, wide, normed, triple, tags, mixed, send_sem, recv_sem,
):
    features = normed.shape[1]
    finish = exchange_halo(plan, edge_ref, wide, send_sem, recv_sem)
    wide[: plan.own_rows, :] = own_ref[...]
    finish()
    arrange_windows(plan, wide, gather_ref, gain_ref, normed, tags)
    attend_windows(plan, inward_ref, bias_ref, normed, triple, tags, mixed, 4)
    own_mixed = pick(scatter_ref[...], mixed[...])
    update = lax.dot_general(own_mixed, outward_ref[0], NT, preferred_element_type=jnp.float32)
    out_ref[...] = (own_ref[:, :features].astype(jnp.float32) + update).astype(jnp.bfloat16)


def level_scratch(plan, features):
    rows = plan.windows * ROWS
    return [
        pltpu.VMEM((plan.wide_rows, features + LANES), jnp.bfloat16),
        pltpu.VMEM((rows, features), jnp.bfloat16),
        pltpu.VMEM((3, rows, features), jnp.bfloat16),
        pltpu.VMEM((rows, LANES), jnp.bfloat16),
        pltpu.VMEM((rows, features), jnp.bfloat16),
        pltpu.SemaphoreType.DMA((len(AROUND),)),
        pltpu.SemaphoreType.DMA((len(AROUND),)),
    ]


class Gather:
    def __init__(self, shards, fulls, split, sems):
        self.shards, self.fulls, self.split, self.sems = shards, fulls, split, sems
        self.entries = weight_entries(shards)
        self.count = len(self.entries)
        self.index = {a: lax.axis_index(a) for a in ("grp", "lat", "lon", "lvl")}
        self.size = {a: lax.axis_size(a) for a in ("grp", "lat", "lon", "lvl")}
        self.halves = 2 if split else 1
        self.ways = [(d, half) for d in range(1, self.size["lon"]) for half in range(self.halves)]

    def at(self, axis, step):
        return {axis: lax.rem(self.index[axis] + step, self.size[axis])}

    def greeted(self):
        axes = ("lon", "lvl", "lat", "grp") if self.split else ("lon", "lvl")
        return [self.at(axis, d) for axis in axes for d in range(1, self.size[axis])]

    def place(self, n, lon_of, start, size):
        m, k, depth = self.entries[n]
        rows, cols = self.shards[m].shape[1:]
        return self.fulls[m].at[
            pl.ds(k, depth),
            pl.ds(pl.multiple_of(lon_of * rows + start, 16), size),
            pl.ds(pl.multiple_of(self.index["lvl"] * cols, cols), cols),
        ]

    def held(self, n, start, size):
        m, k, depth = self.entries[n]
        return self.shards[m].at[pl.ds(k, depth), pl.ds(start, size), :]

    def rows(self, n):
        return self.shards[self.entries[n][0]].shape[1]

    def source(self, d):
        return lax.rem(self.index["lon"] - d + self.size["lon"], self.size["lon"])

    def remote(self, src, dst, kind, number, device):
        send, recv = self.sems[1 + 2 * kind], self.sems[2 + 2 * kind]
        return pltpu.make_async_remote_copy(
            src_ref=src, dst_ref=dst, send_sem=send.at[number], recv_sem=recv.at[number],
            device_id=device, device_id_type=MESH,
        )

    def piece(self, n, half, grp_of, lat_of):
        rows = self.rows(n)
        if not self.split:
            return 0, rows
        grps, lats = self.size["grp"], self.size["lat"]
        size = rows // (2 * grps * lats)
        order = grp_of * lats + lat_of if half == 0 else lat_of * grps + grp_of
        start = half * (rows // 2) + order * size
        return pl.multiple_of(start, 16), size

    def mine(self, n, half):
        return self.piece(n, half, self.index["grp"], self.index["lat"])

    def axis_of(self, half, first):
        return "lat" if (half == 0) == first else "grp"

    def others(self, half, first):
        return range(1, self.size[self.axis_of(half, first)]) if self.split else ()

    def own_copy(self, n):
        return pltpu.make_async_copy(
            self.held(n, 0, self.rows(n)), self.place(n, self.index["lon"], 0, self.rows(n)), self.sems[0].at[n]
        )

    def lon_copy(self, n, d, half):
        start, size = self.mine(n, half)
        return self.remote(
            self.held(n, start, size), self.place(n, self.index["lon"], start, size),
            0, (n, d - 1, half), self.at("lon", d),
        )

    def one_copy(self, n, d, half, e):
        start, size = self.mine(n, half)
        block = self.place(n, self.source(d), start, size)
        return self.remote(block, block, 1, (n, d - 1, half, e - 1), self.at(self.axis_of(half, True), e))

    def two_copy(self, n, d, half, e):
        if half == 0:
            start, size = self.piece(n, half, self.index["grp"], 0)
            size *= self.size["lat"]
        else:
            start, size = self.piece(n, half, 0, self.index["lat"])
            size *= self.size["grp"]
        block = self.place(n, self.source(d), start, size)
        return self.remote(block, block, 2, (n, d - 1, half, e - 1), self.at(self.axis_of(half, False), e))

    def lvl_copy(self, n, d, e):
        block = self.place(n, self.source(d), 0, self.rows(n))
        src = block if d else self.held(n, 0, self.rows(n))
        return self.remote(src, block, 3, (n, d, e - 1), self.at("lvl", e))

    def siblings(self):
        return range(1, self.size["lvl"])

    def begin(self):
        for n in range(self.count):
            self.own_copy(n).start()
            for d, half in self.ways:
                self.lon_copy(n, d, half).start()
            for e in self.siblings():
                self.lvl_copy(n, 0, e).start()

    def step(self, s):
        if s < self.count:
            for d, half in self.ways:
                self.lon_copy(s, d, half).wait_recv()
                for e in self.others(half, True):
                    self.one_copy(s, d, half, e).start()
        if 0 <= s - 1 < self.count:
            for d, half in self.ways:
                for e in self.others(half, True):
                    self.one_copy(s - 1, d, half, e).wait_recv()
                for e in self.others(half, False):
                    self.two_copy(s - 1, d, half, e).start()
        if 0 <= s - 2 < self.count:
            for d in range(1, self.size["lon"]):
                for half in range(self.halves):
                    for e in self.others(half, False):
                        self.two_copy(s - 2, d, half, e).wait_recv()
                for e in self.siblings():
                    self.lvl_copy(s - 2, d, e).start()

    def ready(self, n):
        self.own_copy(n).wait()
        for d in range(self.size["lon"]):
            for e in self.siblings():
                self.lvl_copy(n, d, e).wait_recv()

    def end(self):
        for n in range(self.count):
            for d in range(self.size["lon"]):
                for e in self.siblings():
                    self.lvl_copy(n, d, e).wait_send()
            for d, half in self.ways:
                self.lon_copy(n, d, half).wait_send()
                for e in self.others(half, True):
                    self.one_copy(n, d, half, e).wait_send()
                for e in self.others(half, False):
                    self.two_copy(n, d, half, e).wait_send()


def weight_entries(weights):
    result = []
    for m, w in enumerate(weights):
        each = w.shape[0] if m == 0 else 1
        result += [(m, k, each) for k in range(0, w.shape[0], each)]
    return result


def gather_scratch(weights, split):
    grps, lats, lons, lvls = (lax.axis_size(a) for a in ("grp", "lat", "lon", "lvl"))
    count = len(weight_entries(weights))
    halves = 2 if split else 1
    most = max(grps, lats) - 1 if split else 1
    dma = pltpu.SemaphoreType.DMA
    return (
        [dma((count,))]
        + [dma((count, lons - 1, halves))] * 2
        + [dma((count, lons - 1, halves, most))] * 4
        + [dma((count, lons, lvls - 1))] * 2
    )


def offset_numbers():
    p = np.arange(WIN)
    r, c = p // WIN_LON, p % WIN_LON
    number = (r[:, None] - r[None, :] + WIN_LAT - 1) * (2 * WIN_LON - 1) + c[:, None] - c[None, :] + WIN_LON - 1
    result = np.full((ROWS, LANES), -1, np.int32)
    result[:WIN, :WIN] = number
    return result


def table_parts(table):
    terms, rest = [], table
    for _ in range(3):
        term = lax.reduce_precision(rest, 8, 7)
        terms.append(term.astype(jnp.bfloat16))
        rest = rest - term
    parts = jnp.concatenate(terms, axis=0)
    return jnp.pad(parts, ((0, 0), (0, up_to(parts.shape[1], LANES) - parts.shape[1])))


def shards(
    tokens, fine_tags, coarse_tags, fine_gain, fine_inward, fine_outward, fine_table, merge_gain,
    merge_weight, coarse_gain, coarse_inward, coarse_outward, coarse_table,
):
    _, lat_len, lon_len, width = tokens.shape
    fine_plan, coarse_plan = Plan(lat_len, lon_len), Plan(lat_len // 2, lon_len // 2)
    weights = [fine_inward, fine_outward[None], merge_weight[None], coarse_inward, coarse_outward[None]]
    grps, lats, lons, lvls = (lax.axis_size(a) for a in ("grp", "lat", "lon", "lvl"))
    split = all(w.shape[1] % (2 * grps * lats * 16) == 0 for w in weights)
    wholes = [(w.shape[0], w.shape[1] * lons, w.shape[2] * lvls) for w in weights]

    tagged = jnp.concatenate(
        [tokens[0], jnp.broadcast_to(fine_tags[0, :, :, None], (lat_len, lon_len, LANES)).astype(jnp.bfloat16)], axis=2
    )
    own = tagged.reshape(lat_len * lon_len, -1)
    own = jnp.pad(own, ((0, fine_plan.own_rows - fine_plan.own), (0, 0)))
    pieces = []
    for dy, dx in AROUND:
        part = tagged
        part = part[-HALF_LAT:] if dy < 0 else (part[:HALF_LAT] if dy > 0 else part)
        part = part[:, -HALF_LON:] if dx < 0 else (part[:, :HALF_LON] if dx > 0 else part)
        part = part.reshape(-1, part.shape[2])
        pieces.append(jnp.pad(part, ((0, up_to(part.shape[0], 16) - part.shape[0]), (0, 0))))
    edge = jnp.concatenate(pieces, axis=0)
    coarse_width = wholes[2][1]
    coarse_marks = jnp.broadcast_to(coarse_tags.reshape(-1, 1), (coarse_plan.own, LANES)).astype(jnp.bfloat16)
    coarse_marks = jnp.pad(coarse_marks, ((0, coarse_plan.own_rows - coarse_plan.own), (0, 0)))

    edge_rows = coarse_plan.wide_rows - coarse_plan.own_rows
    heads, coarse_heads = fine_table.shape[0], coarse_table.shape[0]
    fine, coarse_own, coarse_edge, coarse_bias, inward_two, outward_two = pl.pallas_call(
        functools.partial(fine_kernel, fine_plan, split),
        out_shape=[
            jax.ShapeDtypeStruct((fine_plan.own_rows, width), jnp.bfloat16),
            jax.ShapeDtypeStruct((coarse_plan.own_rows, coarse_width + LANES), jnp.bfloat16),
            jax.ShapeDtypeStruct((edge_rows, coarse_width + LANES), jnp.bfloat16),
            jax.ShapeDtypeStruct((coarse_heads, ROWS, LANES), jnp.float32),
            jax.ShapeDtypeStruct(wholes[3], jnp.bfloat16),
            jax.ShapeDtypeStruct(wholes[4], jnp.bfloat16),
        ],
        in_specs=[VMEM] * 12 + [ANY] * 5,
        out_specs=[VMEM] * 6,
        scratch_shapes=level_scratch(fine_plan, width)
        + [pltpu.VMEM((heads, ROWS, LANES), jnp.float32)]
        + [pltpu.VMEM(shape, jnp.bfloat16) for shape in wholes[:3]]
        + gather_scratch(weights, split),
        compiler_params=pltpu.CompilerParams(collective_id=1, has_side_effects=True, vmem_limit_bytes=LIMIT),
        name="fine_level",
    )(
        own, edge, coarse_marks, fine_plan.gather, fine_plan.scatter, fine_plan.patches(),
        coarse_plan.edges(), fine_gain[None], offset_numbers(), table_parts(fine_table),
        table_parts(coarse_table), merge_gain[None], *weights,
    )
    coarse = pl.pallas_call(
        functools.partial(coarse_kernel, coarse_plan),
        out_shape=jax.ShapeDtypeStruct((coarse_plan.own_rows, coarse_width), jnp.bfloat16),
        in_specs=[VMEM] * 8,
        out_specs=VMEM,
        scratch_shapes=level_scratch(coarse_plan, coarse_width),
        compiler_params=pltpu.CompilerParams(collective_id=2, has_side_effects=True, vmem_limit_bytes=LIMIT),
        name="coarse_level",
    )(
        coarse_own, coarse_edge, coarse_plan.gather, coarse_plan.scatter, coarse_gain[None],
        inward_two, outward_two, coarse_bias,
    )
    fine = fine[: fine_plan.own].reshape(tokens.shape)
    coarse = coarse[: coarse_plan.own].reshape(1, lat_len // 2, lon_len // 2, coarse_width)
    return fine, coarse


def solution(mesh):
    placed = (
        P(("grp", "lvl"), "lat", "lon", None),
        P(("grp", "lvl"), "lat", "lon"),
        P(("grp", "lvl"), "lat", "lon"),
        P(),
        P(None, "lon", "lvl"),
        P("lon", "lvl"),
        P(),
        P(),
        P("lon", "lvl"),
        P(),
        P(None, "lon", "lvl"),
        P("lon", "lvl"),
        P(),
    )
    return jax.shard_map(
        shards,
        mesh=mesh,
        in_specs=placed,
        out_specs=(P(("grp", "lvl"), "lat", "lon", None), P(("grp", "lvl"), "lat", "lon", None)),
        check_vma=False,
    )
```
